16 devices in a mesh: rep: 4 (over y, z, core), dp: 4 (over x).
Axes of the slice: x: 4, y: 2, z: 1, core: 2. Of those that a mesh axis runs over, the one named last changes fastest.
The devices are a block of a 4x4x8 slice.
Arguments:
- x: bfloat16 [16, 4096, 896], P(('rep', 'dp')), parts along dimension 0
- dy: bfloat16 [16, 4096, 896], P(('rep', 'dp')), parts along dimension 0
- w_gate: bfloat16 [2, 896, 2560], P(None, 'dp')
- w_up: bfloat16 [2, 896, 2560], P(None, 'dp')
- w_down: bfloat16 [2, 2560, 896], P(None, 'dp')
- m_w_gate: float32 [2, 896, 2560], P(None, 'dp')
- m_w_up: float32 [2, 896, 2560], P(None, 'dp')
- m_w_down: float32 [2, 2560, 896], P(None, 'dp')
- v_w_gate: float32 [2, 896, 2560], P(None, 'dp')
- v_w_up: float32 [2, 896, 2560], P(None, 'dp')
- v_w_down: float32 [2, 2560, 896], P(None, 'dp')
Outputs:
- output 1: bfloat16 [8, 896, 2560], P('rep', 'dp'), parts along dimension 0
- output 2: bfloat16 [8, 896, 2560], P('rep', 'dp'), parts along dimension 0
- output 3: bfloat16 [8, 2560, 896], P('rep', 'dp'), parts along dimension 0
- output 4: float32 [8, 896, 2560], P('rep', 'dp'), parts along dimension 0
- output 5: float32 [8, 896, 2560], P('rep', 'dp'), parts along dimension 0
- output 6: float32 [8, 2560, 896], P('rep', 'dp'), parts along dimension 0
- output 7: float32 [8, 896, 2560], P('rep', 'dp'), parts along dimension 0
- output 8: float32 [8, 896, 2560], P('rep', 'dp'), parts along dimension 0
- output 9: float32 [8, 2560, 896], P('rep', 'dp'), parts along dimension 0
There are 4 independent parts. The reference program is written for one: setup_inputs(seed, part) draws one part's arguments, and reference() takes and returns one part's arrays. A program takes and returns all parts, laid end to end along the dimension named above; an argument that names none is the same for every part.
All inputs are finite; a program needn't handle non-finite values.
Results may differ from the reference program's by a relative error of at most 0.022.
Values are sent between devices in bfloat16 or wider.
A program may use at most 768 MiB of HBM per device.

```python
import jax
import jax.numpy as jnp
from jax import lax

SEQUENCES = 4
TOKENS = 4096
D = 896
FF = 2560
LAYERS = 2
NAMES = ("w_gate", "w_up", "w_down")
SHAPES = {"w_gate": (LAYERS, D, FF), "w_up": (LAYERS, D, FF), "w_down": (LAYERS, FF, D)}


def bump(key, n, height):
    away = (jnp.arange(n, dtype=jnp.int32) - jax.random.randint(key, (), 0, n, jnp.int32)) % n
    return jnp.where(away < n // 8, height, 1.0)


def together(key, own, strength):
    shared = jax.random.normal(key, own.shape[1:], jnp.float32)
    return (own + strength * shared) * lax.rsqrt(1 + strength * strength)


def setup_inputs(seed: int = 0, part: int = 0) -> dict:
    kx, kdy, ka, kb, kz, kf, kh, kl, *keys = jax.random.split(jax.random.key(seed), 8 + 3 * len(NAMES))
    kx, kdy, ka, kb = (jax.random.fold_in(k, part) for k in (kx, kdy, ka, kb))
    kw, km, kv = (keys[i::3] for i in range(3))
    shape = (SEQUENCES, TOKENS, D)
    much_x, much_dy = jax.random.uniform(kz, (2,), jnp.float32, 0.0, 1.0)
    loud = 2.0 ** jax.random.uniform(jax.random.fold_in(kz, 1), (), jnp.float32, -1.0, 2.0)
    layers = 2.0 ** jax.random.uniform(kl, (LAYERS, 1, 1), jnp.float32, -1.0, 1.0)
    x = together(ka, jax.random.normal(kx, shape, jnp.float32), much_x) * bump(kf, D, 4.0)
    dy = together(kb, jax.random.normal(kdy, shape, jnp.float32), much_dy)
    drawn = {"x": x.astype(jnp.bfloat16), "dy": (loud * dy * (SEQUENCES * TOKENS) ** -0.5).astype(jnp.bfloat16)}
    for key, name in zip(kw, NAMES, strict=True):
        w = jax.random.normal(key, SHAPES[name], jnp.float32) * SHAPES[name][1] ** -0.5
        drawn[name] = (w * {"w_gate": 1.0, "w_up": bump(kh, FF, 4.0), "w_down": layers}[name]).astype(jnp.bfloat16)
    for key, name in zip(km, NAMES, strict=True):
        drawn[f"m_{name}"] = 0.1 * jax.random.normal(key, SHAPES[name], jnp.float32)
    for key, name in zip(kv, NAMES, strict=True):
        drawn[f"v_{name}"] = jax.random.uniform(key, SHAPES[name], jnp.float32, 0.005, 0.015)
    return drawn


def matmul(a, w):
    return jnp.dot(a, w, preferred_element_type=jnp.float32).astype(jnp.bfloat16)


def normed(h):
    wide = h.astype(jnp.float32)
    scale = lax.rsqrt(jnp.mean(wide**2, -1, keepdims=True) + 1e-6)
    return (wide * scale).astype(jnp.bfloat16)


def layer(h, w):
    a = normed(h)
    gate = jnp.dot(a, w["w_gate"], preferred_element_type=jnp.float32)
    up = jnp.dot(a, w["w_up"], preferred_element_type=jnp.float32)
    return h + matmul((jax.nn.silu(gate) * up).astype(jnp.bfloat16), w["w_down"])


def adamw(w, m, v, g):
    m = 0.9 * m + 0.1 * g
    v = 0.95 * v + 0.05 * g * g
    step = m * lax.rsqrt(v + 1e-8) + 0.1 * w
    return (w - 0.02 * step).astype(jnp.bfloat16), m, v


def clipped(gradients, sum_of_squares, count):
    factor = jnp.minimum(1.0, 0.5 * lax.rsqrt(sum_of_squares / count + 1e-30))
    return [g * factor for g in gradients]


def stack(weights, h):
    return lax.scan(lambda h, w: (layer(h, w), None), h, weights)[0]


def reference(x, dy, w_gate, w_up, w_down, m_w_gate, m_w_up, m_w_down, v_w_gate, v_w_up, v_w_down):
    weights = dict(zip(NAMES, (w_gate, w_up, w_down), strict=True))

    def take(so_far, sequence):
        h, by_y = sequence
        _, back = jax.vjp(lambda w: stack(w, h), weights)
        return jax.tree.map(lambda total, term: total + term.astype(jnp.float32), so_far, back(by_y)[0]), None

    none_yet = {name: jnp.zeros(w.shape, jnp.float32) for name, w in weights.items()}
    by_weights, _ = lax.scan(take, none_yet, (x, dy))
    gradients = [by_weights[name].astype(jnp.bfloat16).astype(jnp.float32) for name in NAMES]
    gradients = clipped(gradients, sum(jnp.sum(g * g) for g in gradients), sum(g.size for g in gradients))
    new = [
        adamw(w.astype(jnp.float32), m, v, g)
        for w, m, v, g in zip((w_gate, w_up, w_down), (m_w_gate, m_w_up, m_w_down), (v_w_gate, v_w_up, v_w_down), gradients, strict=True)
    ]
    return tuple(one[which] for which in range(3) for one in new)
```

```python
import functools

import jax
import jax.numpy as jnp
from jax import lax
from jax.experimental import pallas as pl
from jax.experimental.pallas import tpu as pltpu
from jax.sharding import PartitionSpec as P

MESH = pl.DeviceIdType.MESH
ANY = pl.BlockSpec(memory_space=pl.ANY)
F32, BF16 = jnp.float32, jnp.bfloat16
VMEM_LIMIT = 60 * 1024 * 1024
ROWS = 512
COLS = 256


def dot(a, b, dims=((1,), (0,))):
    return lax.dot_general(a, b, (dims, ((), ())), preferred_element_type=F32)


NT = ((1,), (1,))


def inv_rms(wide):
    return lax.rsqrt(jnp.mean(wide * wide, -1, keepdims=True) + 1e-6)


def normed(h):
    wide = h.astype(F32)
    return (wide * inv_rms(wide)).astype(BF16)


class Gather:
    def __init__(self, n, shards, fulls, stages, local_sem, send_sem, recv_sem):
        self.me, rep = lax.axis_index("dp"), lax.axis_index("rep")
        self.n, self.p = n, lax.rem(rep, 2)
        self.right, self.left = {"dp": lax.rem(self.me + 1, n)}, {"dp": lax.rem(self.me + n - 1, n)}
        self.partner = {"rep": rep + 1 - 2 * self.p}
        self.shards, self.fulls, self.stages = shards, fulls, stages
        self.local_sem, self.send_sem, self.recv_sem = local_sem, send_sem, recv_sem

    def barrier(self):
        sem = pltpu.get_barrier_semaphore()
        for device in (self.left, self.right, self.partner):
            pl.semaphore_signal(sem, inc=1, device_id=device, device_id_type=MESH)
        pl.semaphore_wait(sem, 3)

    def half(self, k, away, part=None):
        rows, columns = self.shards[k].shape
        owner = lax.rem(self.me + away + self.n, self.n)
        start = pl.multiple_of(owner * rows + self.p * (rows // 2), 16)
        if part is None:
            return self.fulls[k].at[pl.ds(start, rows // 2)]
        if columns % 256 == 0:
            return self.fulls[k].at[pl.ds(start, rows // 2), pl.ds(part * (columns // 2), columns // 2)]
        quarter = rows // 4
        return self.fulls[k].at[pl.ds(pl.multiple_of(start + part * quarter, 16), quarter)]

    def copy(self, k, slot, src, dst, device):
        return pltpu.make_async_remote_copy(src_ref=src, dst_ref=dst, send_sem=self.send_sem.at[k, slot], recv_sem=self.recv_sem.at[k, slot], device_id=device, device_id_type=MESH)

    def first(self, k, side):
        rows = self.shards[k].shape[0]
        own = self.shards[k].at[pl.ds(pl.multiple_of(self.p * (rows // 2), 16), rows // 2)]
        return self.copy(k, side, own, self.half(k, 0), self.left if side else self.right)

    def second(self, k, side):
        place = self.half(k, 1 if side else -1, side)
        return self.copy(k, 2 + side, place, place, self.left if side else self.right)

    def over(self, k, which):
        place = self.half(k, (-1, 1, 2)[which])
        return self.copy(k, 4 + which, place, place, self.partner)

    def load(self, k):
        return pltpu.make_async_copy(self.shards[k], self.stages[k], self.local_sem.at[k, 0])

    def store(self, k):
        rows = self.shards[k].shape[0]
        place = self.fulls[k].at[pl.ds(pl.multiple_of(self.me * rows, 16), rows)]
        return pltpu.make_async_copy(self.stages[k], place, self.local_sem.at[k, 1])

    def start(self, k):
        self.first(k, 0).start()
        self.first(k, 1).start()
        self.load(k).start()

    def keep(self, k):
        self.load(k).wait()
        self.store(k).start()

    def forward(self, k):
        for side in (0, 1):
            self.first(k, side).wait_recv()
            self.second(k, side).start()
        self.over(k, 0).start()
        self.over(k, 1).start()

    def last(self, k):
        self.second(k, 0).wait_recv()
        self.second(k, 1).wait_recv()
        self.over(k, 2).start()

    def finish(self, k):
        self.store(k).wait()
        for which in range(3):
            self.over(k, which).wait()
        for side in (0, 1):
            self.first(k, side).wait_send()
            self.second(k, side).wait_send()


def gather_scratch(weights):
    k = len(weights)
    return [pltpu.VMEM(w.shape[1:], w.dtype) for w in weights] + [pltpu.SemaphoreType.DMA((k, 2)), pltpu.SemaphoreType.DMA((k, 7)), pltpu.SemaphoreType.DMA((k, 7))]


def fulls_of(n, weights):
    return [jax.ShapeDtypeStruct((n * w.shape[1], w.shape[2]), w.dtype) for w in weights]


def gather_kernel(n, *refs):
    k = (len(refs) - 3) // 3
    g = Gather(n, [s.at[0] for s in refs[:k]], refs[k : 2 * k], refs[2 * k : 3 * k], *refs[3 * k :])
    g.barrier()
    for phase in (g.start, g.keep, g.forward, g.last, g.finish):
        for one in range(k):
            phase(one)


def gathered(n, weights):
    k = len(weights)
    sent = sum(3 * w.shape[1] * w.shape[2] for w in weights)
    return pl.pallas_call(
        functools.partial(gather_kernel, n),
        out_shape=fulls_of(n, weights),
        in_specs=[ANY] * k,
        out_specs=[ANY] * k,
        scratch_shapes=gather_scratch(weights),
        compiler_params=pltpu.CompilerParams(collective_id=0, has_side_effects=True, vmem_limit_bytes=16 * 1024 * 1024),
        cost_estimate=pl.CostEstimate(flops=40_000_000_000, bytes_accessed=8 * sent, transcendentals=0),
        name="gather",
    )(*weights)


def whole(array):
    return pl.BlockSpec(array.shape, lambda i: (0,) * len(array.shape), pipeline_mode=pl.Buffered(1))


def rows_of(d):
    return pl.BlockSpec((ROWS, d), lambda i: (i, 0))


def columns_of(d):
    return pl.BlockSpec((d, ROWS), lambda i: (0, i))


def part_of(array, dim, half):
    shape = tuple(s // 2 if i == dim else s for i, s in enumerate(array.shape))
    place = tuple(half if i == dim else 0 for i in range(2))
    return pl.BlockSpec(shape, lambda i: place, pipeline_mode=pl.Buffered(1))


def params(**more):
    return pltpu.CompilerParams(dimension_semantics=("arbitrary",), vmem_limit_bytes=VMEM_LIMIT, **more)


def beside(g, k, steps, forwards):
    i = pl.program_id(0)

    @pl.when(i == 0)
    def _():
        g.barrier()
        for one in range(k):
            g.start(one)

    @pl.when(i == 1)
    def _():
        for one in range(k):
            g.keep(one)

    for one, at in enumerate(forwards):

        @pl.when(i == at)
        def _(one=one):
            g.forward(one)


def after(g, k, steps):
    @pl.when(pl.program_id(0) == steps - 1)
    def _():
        for phase in (g.last, g.finish):
            for one in range(k):
                phase(one)


def up_kernel(n, layers, steps, x_ref, wg_ref, wu_ref, *refs):
    k = len(layers)
    shards, (gate_ref, up_ref, act_ref, at_ref), refs = refs[:k], refs[k : k + 4], refs[k + 4 :]
    g = Gather(n, [s.at[layer] for s, layer in zip(shards, layers)], refs[:k], refs[k : 2 * k], *refs[2 * k :])
    beside(g, k, steps, (2, 5))
    a = normed(x_ref[...])
    at_ref[...] = a.T
    for c in range(wg_ref.shape[1] // COLS):
        cols = pl.ds(c * COLS, COLS)
        gate = dot(a, wg_ref[:, cols])
        up = dot(a, wu_ref[:, cols])
        gate_ref[:, cols] = gate
        up_ref[:, cols] = up
        act_ref[:, cols] = (gate * jax.nn.sigmoid(gate) * up).astype(BF16)
    after(g, k, steps)


def up_part(n, x, full, weights, layers):
    tokens, d = x.shape
    ff, k = full[0].shape[1], len(weights)
    steps = tokens // ROWS
    wide = jax.ShapeDtypeStruct((tokens, ff), F32)
    return pl.pallas_call(
        functools.partial(up_kernel, n, layers, steps),
        grid=(steps,),
        out_shape=[wide, wide, jax.ShapeDtypeStruct((tokens, ff), BF16), jax.ShapeDtypeStruct((d, tokens), BF16), *fulls_of(n, weights)],
        in_specs=[rows_of(d), whole(full[0]), whole(full[1])] + [ANY] * k,
        out_specs=[rows_of(ff)] * 3 + [columns_of(d)] + [ANY] * k,
        scratch_shapes=gather_scratch(weights),
        compiler_params=params(collective_id=1, has_side_effects=True),
        cost_estimate=pl.CostEstimate(flops=4 * tokens * d * ff, bytes_accessed=10 * tokens * ff, transcendentals=tokens * ff),
        name="up",
    )(x, *full, *weights)


def down_kernel(n, layers, steps, x_ref, act_ref, wd_ref, *refs):
    k = len(layers)
    shards, (h_ref, at_ref), refs = refs[:k], refs[k : k + 2], refs[k + 2 :]
    g = Gather(n, [s.at[layer] for s, layer in zip(shards, layers)], refs[:k], refs[k : 2 * k], *refs[2 * k :])
    beside(g, k, steps, (4, 7))
    h = x_ref[...] + dot(act_ref[...], wd_ref[...]).astype(BF16)
    h_ref[...] = h
    at_ref[...] = normed(h).T
    after(g, k, steps)


def down_part(n, x, act, full, weights, layers):
    tokens, d = x.shape
    ff, k = act.shape[1], len(weights)
    steps = tokens // ROWS
    return pl.pallas_call(
        functools.partial(down_kernel, n, layers, steps),
        grid=(steps,),
        out_shape=[jax.ShapeDtypeStruct((tokens, d), BF16), jax.ShapeDtypeStruct((d, tokens), BF16), *fulls_of(n, weights)],
        in_specs=[rows_of(d), rows_of(ff), whole(full)] + [ANY] * k,
        out_specs=[rows_of(d), columns_of(d)] + [ANY] * k,
        scratch_shapes=gather_scratch(weights),
        compiler_params=params(collective_id=2, has_side_effects=True),
        cost_estimate=pl.CostEstimate(flops=2 * tokens * d * ff, bytes_accessed=2 * tokens * ff + 6 * tokens * d, transcendentals=0),
        name="down",
    )(x, act, full, *weights)


def by_hidden(gate, up, dact, s):
    silu = gate * s
    return (dact * up * (s + silu * (1 - s))).astype(BF16), (dact * silu).astype(BF16)


def hidden_kernel(h_ref, dy_ref, wg_ref, wu_ref, wd_ref, act_ref, dg_ref, du_ref, *dyt_ref):
    a, dy = normed(h_ref[...]), dy_ref[...]
    for ref in dyt_ref:
        ref[...] = dy.T
    for c in range(wg_ref.shape[1] // COLS):
        cols = pl.ds(c * COLS, COLS)
        gate = dot(a, wg_ref[:, cols])
        up = dot(a, wu_ref[:, cols])
        dact = dot(dy, wd_ref[cols, :], NT).astype(BF16).astype(F32)
        s = jax.nn.sigmoid(gate)
        act_ref[:, cols] = (gate * s * up).astype(BF16)
        dg_ref[:, cols], du_ref[:, cols] = by_hidden(gate, up, dact, s)


def hidden(h, dy, full, half):
    tokens, d = h.shape
    ff = full[0].shape[1] // 2
    wide = jax.ShapeDtypeStruct((tokens, ff), BF16)
    return pl.pallas_call(
        hidden_kernel,
        grid=(tokens // ROWS,),
        out_shape=[wide] * 3 + [jax.ShapeDtypeStruct((d, tokens), BF16)] * half,
        in_specs=[rows_of(d), rows_of(d), part_of(full[0], 1, half), part_of(full[1], 1, half), part_of(full[2], 0, half)],
        out_specs=[rows_of(ff)] * 3 + [columns_of(d)] * half,
        compiler_params=params(),
        cost_estimate=pl.CostEstimate(flops=6 * tokens * d * ff, bytes_accessed=4 * tokens * d + 6 * tokens * ff + 6 * d * ff, transcendentals=tokens * ff),
        name="hidden",
    )(h, dy, *full)


def kept_kernel(gate_ref, up_ref, dy_ref, wd_ref, dg_ref, du_ref):
    dy = dy_ref[...]
    for c in range(gate_ref.shape[1] // COLS):
        cols = pl.ds(c * COLS, COLS)
        gate = gate_ref[:, cols]
        dact = dot(dy, wd_ref[cols, :], NT).astype(BF16).astype(F32)
        dg_ref[:, cols], du_ref[:, cols] = by_hidden(gate, up_ref[:, cols], dact, jax.nn.sigmoid(gate))


def kept_hidden(gate, up, dy, full, half):
    tokens, d = dy.shape
    ff = gate.shape[1] // 2
    wide = jax.ShapeDtypeStruct((tokens, ff), BF16)
    block = pl.BlockSpec((ROWS, ff), lambda i: (i, half))
    return pl.pallas_call(
        kept_kernel,
        grid=(tokens // ROWS,),
        out_shape=[wide] * 2,
        in_specs=[block, block, rows_of(d), part_of(full, 0, half)],
        out_specs=[rows_of(ff)] * 2,
        compiler_params=params(),
        cost_estimate=pl.CostEstimate(flops=2 * tokens * d * ff, bytes_accessed=2 * tokens * d + 12 * tokens * ff + 2 * d * ff, transcendentals=tokens * ff),
        name="kept_hidden",
    )(gate, up, dy, full)


def gradient_kernel(turn, counts, at_ref, *refs):
    k = len(counts)
    i, first = pl.program_id(0), 0
    for one, count in enumerate(counts):

        @pl.when(jnp.logical_and(i >= first, i < first + count))
        def _(d_ref=refs[one]):
            out = dot(at_ref[...], d_ref[...])
            refs[k][...] = (out.T if turn else out).astype(BF16)

        first += count


def gradient(at, ds, turn=False):
    rows, tokens = at.shape
    cols = 256
    counts = [d.shape[1] // cols for d in ds]
    firsts = [sum(counts[:one]) for one in range(len(ds))]
    ff = sum(d.shape[1] for d in ds)

    def along(height, one):
        return pl.BlockSpec((height, cols), lambda i: (0, jnp.clip(i - firsts[one], 0, counts[one] - 1)))

    shape, out = (ff, rows), pl.BlockSpec((cols, rows), lambda i: (i, 0))
    if not turn:
        shape, out = (rows, ff), pl.BlockSpec((rows, cols), lambda i: (0, i))
    return pl.pallas_call(
        functools.partial(gradient_kernel, turn, counts),
        grid=(sum(counts),),
        out_shape=jax.ShapeDtypeStruct(shape, BF16),
        in_specs=[whole(at)] + [along(tokens, one) for one in range(len(ds))],
        out_specs=out,
        compiler_params=params(),
        cost_estimate=pl.CostEstimate(flops=2 * tokens * rows * ff, bytes_accessed=2 * (rows * tokens + ff * tokens + rows * ff), transcendentals=0),
        name="gradient",
    )(at, *ds)


def states_kernel(dga_ref, dgb_ref, dua_ref, dub_ref, h_ref, dy_ref, wg_ref, wu_ref, dh_ref, dht_ref):
    ff = dga_ref.shape[1]

    def through(a_ref, b_ref, w_ref):
        return (dot(a_ref[...], w_ref[:, :ff], NT) + dot(b_ref[...], w_ref[:, ff:], NT)).astype(BF16)

    da = (through(dga_ref, dgb_ref, wg_ref) + through(dua_ref, dub_ref, wu_ref)).astype(F32)
    wide = h_ref[...].astype(F32)
    scale = inv_rms(wide)
    by_scale = jnp.sum(da * wide, -1, keepdims=True)
    dh = da * scale - (by_scale * scale * scale * scale / wide.shape[-1]) * wide
    dh = dy_ref[...] + dh.astype(BF16)
    dh_ref[...] = dh
    dht_ref[...] = dh.T


def states(dg, du, h, dy, full):
    tokens, d = h.shape
    ff = dg[0].shape[1]
    return pl.pallas_call(
        states_kernel,
        grid=(tokens // ROWS,),
        out_shape=[jax.ShapeDtypeStruct((tokens, d), BF16), jax.ShapeDtypeStruct((d, tokens), BF16)],
        in_specs=[rows_of(ff)] * 4 + [rows_of(d), rows_of(d), whole(full[0]), whole(full[1])],
        out_specs=[rows_of(d), columns_of(d)],
        compiler_params=params(),
        cost_estimate=pl.CostEstimate(flops=8 * tokens * d * ff, bytes_accessed=8 * tokens * ff + 8 * tokens * d + 8 * d * ff, transcendentals=tokens),
        name="states",
    )(*dg, *du, h, dy, full[0], full[1])


def adamw(w, m, v, g):
    m = 0.9 * m + 0.1 * g
    v = 0.95 * v + 0.05 * g * g
    step = m * lax.rsqrt(v + 1e-8) + 0.1 * w
    return (w - 0.02 * step).astype(BF16), m, v


def clipped(gradients, sum_of_squares, count):
    factor = jnp.minimum(1.0, 0.5 * lax.rsqrt(sum_of_squares / count + 1e-30))
    return [g * factor for g in gradients]


def solution(mesh):
    n = mesh.shape["dp"]

    def scattered(g):
        return lax.psum_scatter(g, "dp", scatter_dimension=0, tiled=True)

    def follow(array, *earlier):
        return lax.optimization_barrier((array, *earlier))[0]

    def step(x, dy, *arrays):
        weights, m, v = (arrays[i : i + 3] for i in (0, 3, 6))
        x, dy = x[0], dy[0]
        w_gate, w_up, w_down = weights
        full = gathered(n, (w_gate, w_up))
        gate, up, act, at0, down0, gate1 = up_part(n, x, full, (w_down, w_gate), (0, 1))
        h, at1, up1, down1 = down_part(n, x, act, down0, (w_up, w_down), (1, 1))
        full1 = gate1, up1, down1

        act_a, dg_a, du_a = hidden(h, dy, full1, 0)
        one_a = gradient(at1, (dg_a, du_a))
        sum_a = scattered(one_a)
        act_b, dg_b, du_b, dyt = hidden(follow(h, one_a), dy, full1, 1)
        one_b = gradient(at1, (dg_b, du_b))
        sum_b = scattered(one_b)
        one_down = gradient(follow(dyt, one_b), (act_a, act_b), True)
        sum_down = scattered(one_down)
        dh, dht = states((dg_a, dg_b), (du_a, du_b), follow(h, one_down, sum_a), dy, full1)
        down = gradient(dht, (act,), True)
        last_down = scattered(down)
        dg_a, du_a = kept_hidden(gate, up, follow(dh, down, sum_b), down0, 0)
        a = gradient(at0, (dg_a, du_a))
        last_a = scattered(a)
        dg_b, du_b = kept_hidden(gate, up, follow(dh, a, sum_down), down0, 1)
        last_b = scattered(gradient(follow(at0, last_down), (dg_b, du_b)))

        sums = sum_a, sum_b, sum_down, last_down, last_a, last_b
        squares = lax.psum(sum(jnp.sum(lax.optimization_barrier(g).astype(F32) ** 2) for g in sums), "dp")

        def joined(a, b, side):
            half = a.shape[1] // 2
            return jnp.concatenate([one[:, side * half : (side + 1) * half] for one in (a, b)], -1)

        pairs = (last_a, last_b), (sum_a, sum_b)
        gradients = [jnp.stack([joined(a, b, side) for a, b in pairs]).astype(F32) for side in range(2)]
        gradients.append(jnp.stack([last_down, sum_down]).astype(F32))
        gradients = clipped(gradients, squares, lax.psum(1, "dp") * sum(g.size for g in gradients))
        new = [adamw(w.astype(F32), m, v, g) for w, m, v, g in zip(weights, m, v, gradients, strict=True)]
        return tuple(one[which] for which in range(3) for one in new)

    spec, cut = P(("rep", "dp"), None, None), P(None, "dp", None)
    return jax.shard_map(
        step,
        mesh=mesh,
        in_specs=(spec, spec) + (cut,) * 9,
        out_specs=(P("rep", "dp", None),) * 9,
        check_vma=False,
    )
```

```python
import functools

import jax
import jax.numpy as jnp
from jax import lax
from jax.experimental import pallas as pl
from jax.experimental.pallas import tpu as pltpu
from jax.sharding import PartitionSpec as P

MESH = pl.DeviceIdType.MESH
ANY = pl.BlockSpec(memory_space=pl.ANY)
F32, BF16 = jnp.float32, jnp.bfloat16
VMEM_LIMIT = 60 * 1024 * 1024
ROWS = 512
COLS = 256


def dot(a, b, dims=((1,), (0,))):
    return lax.dot_general(a, b, (dims, ((), ())), preferred_element_type=F32)


NT = ((1,), (1,))


def inv_rms(wide):
    return lax.rsqrt(jnp.mean(wide * wide, -1, keepdims=True) + 1e-6)


def normed(h):
    wide = h.astype(F32)
    return (wide * inv_rms(wide)).astype(BF16)


class Gather:
    def __init__(self, n, shards, fulls, stages, local_sem, send_sem, recv_sem):
        self.me, rep = lax.axis_index("dp"), lax.axis_index("rep")
        self.n, self.p, self.b = n, lax.rem(rep, 2), lax.rem(rep // 2, 2)
        self.right, self.left = {"dp": lax.rem(self.me + 1, n)}, {"dp": lax.rem(self.me + n - 1, n)}
        self.partner, self.sharer = {"rep": rep + 1 - 2 * self.p}, {"rep": rep + 2 - 4 * self.b}
        self.shards, self.fulls, self.stages = shards, fulls, stages
        self.local_sem, self.send_sem, self.recv_sem = local_sem, send_sem, recv_sem

    def barrier(self):
        sem = pltpu.get_barrier_semaphore()
        for device in (self.left, self.right, self.partner, self.sharer):
            pl.semaphore_signal(sem, inc=1, device_id=device, device_id_type=MESH)
        pl.semaphore_wait(sem, 4)

    def cut(self, k):
        rows, columns = self.shards[k].shape
        wide = columns % 256 == 0
        unit = 128 if wide else 16
        units = columns // unit if wide else rows // 2 // unit
        alone = units * 3 // 10
        return wide, unit, alone, units - 2 * alone

    def place(self, ref, row, k, start, size):
        wide, unit, _, _ = self.cut(k)
        if wide:
            return ref.at[pl.ds(pl.multiple_of(row, 16), self.shards[k].shape[0] // 2), pl.ds(pl.multiple_of(start * unit, unit), size * unit)]
        return ref.at[pl.ds(pl.multiple_of(row + start * unit, 16), size * unit)]

    def there(self, k, away, start, size):
        rows = self.shards[k].shape[0]
        owner = lax.rem(self.me + away + self.n, self.n)
        return self.place(self.fulls[k], owner * rows + self.p * (rows // 2), k, start, size)

    def copy(self, k, slot, src, dst, device):
        return pltpu.make_async_remote_copy(src_ref=src, dst_ref=dst, send_sem=self.send_sem.at[k, slot], recv_sem=self.recv_sem.at[k, slot], device_id=device, device_id_type=MESH)

    def first(self, k, side):
        _, _, alone, both = self.cut(k)
        own = self.place(self.shards[k], self.p * (self.shards[k].shape[0] // 2), k, self.b * alone, alone + both)
        return self.copy(k, side, own, self.there(k, 0, self.b * alone, alone + both), self.left if side else self.right)

    def second(self, k, side):
        _, _, alone, both = self.cut(k)
        size = (alone + both + 1) // 2
        start = self.b * alone + (size if side else 0)
        place = self.there(k, 1 if side else -1, start, alone + both - size if side else size)
        return self.copy(k, 2 + side, place, place, self.left if side else self.right)

    def shared(self, k, which):
        _, _, alone, both = self.cut(k)
        place = self.there(k, (-1, 1, 2)[which], self.b * (alone + both), alone)
        return self.copy(k, 4 + which, place, place, self.sharer)

    def over(self, k, which):
        _, _, alone, both = self.cut(k)
        away = (-1, 1, 2)[which % 3]
        if which < 3:
            place = self.there(k, away, self.b * alone, alone + both)
        else:
            place = self.there(k, away, (1 - self.b) * (alone + both), alone)
        return self.copy(k, 7 + which, place, place, self.partner)

    def load(self, k):
        return pltpu.make_async_copy(self.shards[k], self.stages[k], self.local_sem.at[k, 0])

    def store(self, k):
        rows = self.shards[k].shape[0]
        place = self.fulls[k].at[pl.ds(pl.multiple_of(self.me * rows, 16), rows)]
        return pltpu.make_async_copy(self.stages[k], place, self.local_sem.at[k, 1])

    def start(self, k):
        self.first(k, 0).start()
        self.first(k, 1).start()
        self.load(k).start()

    def keep(self, k):
        self.load(k).wait()
        self.store(k).start()

    def forward(self, k):
        for side in (0, 1):
            self.first(k, side).wait_recv()
            self.second(k, side).start()
            self.shared(k, side).start()
            self.over(k, side).start()

    def last(self, k):
        self.second(k, 0).wait_recv()
        self.second(k, 1).wait_recv()
        self.shared(k, 2).start()
        self.over(k, 2).start()
        for side in (0, 1):
            self.shared(k, side).wait_recv()
            self.over(k, 3 + side).start()

    def end(self, k):
        self.shared(k, 2).wait_recv()
        self.over(k, 5).start()

    def finish(self, k):
        self.store(k).wait()
        for which in range(6):
            self.over(k, which).wait()
        for side in (0, 1):
            self.first(k, side).wait_send()
            self.second(k, side).wait_send()
        for which in range(3):
            self.shared(k, which).wait_send()


def gather_scratch(weights, pieces=1):
    k = len(weights) * pieces
    return [pltpu.VMEM(w.shape[1:], w.dtype) for w in weights] + [pltpu.SemaphoreType.DMA((k, 2)), pltpu.SemaphoreType.DMA((k, 13)), pltpu.SemaphoreType.DMA((k, 13))]


def fulls_of(n, weights):
    return [jax.ShapeDtypeStruct((n * w.shape[1], w.shape[2]), w.dtype) for w in weights]


def gather_kernel(n, *refs):
    k = (len(refs) - 3) // 3
    columns = refs[0].shape[2] // 2
    halves = [pl.ds(half * columns, columns) for half in range(2)]
    shards = [s.at[0, :, half] for s in refs[:k] for half in halves]
    fulls, stages = ([s.at[:, half] for s in some for half in halves] for some in (refs[k : 2 * k], refs[2 * k : 3 * k]))
    g = Gather(n, shards, fulls, stages, *refs[3 * k :])
    g.barrier()
    for phase in (g.start, g.keep, g.forward, g.last, g.end, g.finish):
        for one in range(2 * k):
            phase(one)


def gathered(n, weights):
    k = len(weights)
    sent = sum(3 * w.shape[1] * w.shape[2] for w in weights)
    return pl.pallas_call(
        functools.partial(gather_kernel, n),
        out_shape=fulls_of(n, weights),
        in_specs=[ANY] * k,
        out_specs=[ANY] * k,
        scratch_shapes=gather_scratch(weights, 2),
        compiler_params=pltpu.CompilerParams(collective_id=0, has_side_effects=True, vmem_limit_bytes=16 * 1024 * 1024),
        cost_estimate=pl.CostEstimate(flops=40_000_000_000, bytes_accessed=8 * sent, transcendentals=0),
        name="gather",
    )(*weights)


def whole(array):
    return pl.BlockSpec(array.shape, lambda i: (0,) * len(array.shape), pipeline_mode=pl.Buffered(1))


def rows_of(d):
    return pl.BlockSpec((ROWS, d), lambda i: (i, 0))


def columns_of(d):
    return pl.BlockSpec((d, ROWS), lambda i: (0, i))


def part_of(array, dim, half):
    shape = tuple(s // 2 if i == dim else s for i, s in enumerate(array.shape))
    place = tuple(half if i == dim else 0 for i in range(2))
    return pl.BlockSpec(shape, lambda i: place, pipeline_mode=pl.Buffered(1))


def params(**more):
    return pltpu.CompilerParams(dimension_semantics=("arbitrary",), vmem_limit_bytes=VMEM_LIMIT, **more)


def beside(g, k, steps, times):
    i = pl.program_id(0)
    phases = (g.start, (0,) * k), (g.keep, (1,) * k), *zip((g.forward, g.last), times)
    for phase, steps_of in phases:
        for one, at in enumerate(steps_of):

            @pl.when(i == at)
            def _(phase=phase, one=one):
                if phase == g.start and one == 0:
                    g.barrier()
                phase(one)


def after(g, k, steps):
    @pl.when(pl.program_id(0) == steps - 1)
    def _():
        for phase in (g.end, g.finish):
            for one in range(k):
                phase(one)


def up_kernel(n, layers, steps, x_ref, wg_ref, wu_ref, *refs):
    k = len(layers)
    shards, (gate_ref, up_ref, act_ref, at_ref), refs = refs[:k], refs[k : k + 4], refs[k + 4 :]
    g = Gather(n, [s.at[layer] for s, layer in zip(shards, layers)], refs[:k], refs[k : 2 * k], *refs[2 * k :])
    beside(g, k, steps, ((2, 3, 4), (5, 6, 7)))
    a = normed(x_ref[...])
    at_ref[...] = a.T
    for c in range(wg_ref.shape[1] // COLS):
        cols = pl.ds(c * COLS, COLS)
        gate = dot(a, wg_ref[:, cols])
        up = dot(a, wu_ref[:, cols])
        gate_ref[:, cols] = gate
        up_ref[:, cols] = up
        act_ref[:, cols] = (gate * jax.nn.sigmoid(gate) * up).astype(BF16)
    after(g, k, steps)


def up_part(n, x, full, weights, layers):
    tokens, d = x.shape
    ff, k = full[0].shape[1], len(weights)
    steps = tokens // ROWS
    wide = jax.ShapeDtypeStruct((tokens, ff), F32)
    return pl.pallas_call(
        functools.partial(up_kernel, n, layers, steps),
        grid=(steps,),
        out_shape=[wide, wide, jax.ShapeDtypeStruct((tokens, ff), BF16), jax.ShapeDtypeStruct((d, tokens), BF16), *fulls_of(n, weights)],
        in_specs=[rows_of(d), whole(full[0]), whole(full[1])] + [ANY] * k,
        out_specs=[rows_of(ff)] * 3 + [columns_of(d)] + [ANY] * k,
        scratch_shapes=gather_scratch(weights),
        compiler_params=params(collective_id=1, has_side_effects=True),
        cost_estimate=pl.CostEstimate(flops=4 * tokens * d * ff, bytes_accessed=10 * tokens * ff, transcendentals=tokens * ff),
        name="up",
    )(x, *full, *weights)


def down_kernel(n, layers, steps, x_ref, act_ref, wd_ref, *refs):
    k = len(layers)
    shards, (h_ref, at_ref), refs = refs[:k], refs[k : k + 2], refs[k + 2 :]
    g = Gather(n, [s.at[layer] for s, layer in zip(shards, layers)], refs[:k], refs[k : 2 * k], *refs[2 * k :])
    beside(g, k, steps, ((3,), (6,)))
    h = x_ref[...] + dot(act_ref[...], wd_ref[...]).astype(BF16)
    h_ref[...] = h
    at_ref[...] = normed(h).T
    after(g, k, steps)


def down_part(n, x, act, full, weights, layers):
    tokens, d = x.shape
    ff, k = act.shape[1], len(weights)
    steps = tokens // ROWS
    return pl.pallas_call(
        functools.partial(down_kernel, n, layers, steps),
        grid=(steps,),
        out_shape=[jax.ShapeDtypeStruct((tokens, d), BF16), jax.ShapeDtypeStruct((d, tokens), BF16), *fulls_of(n, weights)],
        in_specs=[rows_of(d), rows_of(ff), whole(full)] + [ANY] * k,
        out_specs=[rows_of(d), columns_of(d)] + [ANY] * k,
        scratch_shapes=gather_scratch(weights),
        compiler_params=params(collective_id=2, has_side_effects=True),
        cost_estimate=pl.CostEstimate(flops=2 * tokens * d * ff, bytes_accessed=2 * tokens * ff + 6 * tokens * d, transcendentals=0),
        name="down",
    )(x, act, full, *weights)


def by_hidden(gate, up, dact, s):
    silu = gate * s
    return (dact * up * (s + silu * (1 - s))).astype(BF16), (dact * silu).astype(BF16)


def hidden_kernel(h_ref, dy_ref, wg_ref, wu_ref, wd_ref, act_ref, dg_ref, du_ref, *dyt_ref):
    a, dy = normed(h_ref[...]), dy_ref[...]
    for ref in dyt_ref:
        ref[...] = dy.T
    for c in range(wg_ref.shape[1] // COLS):
        cols = pl.ds(c * COLS, COLS)
        gate = dot(a, wg_ref[:, cols])
        up = dot(a, wu_ref[:, cols])
        dact = dot(dy, wd_ref[cols, :], NT).astype(BF16).astype(F32)
        s = jax.nn.sigmoid(gate)
        act_ref[:, cols] = (gate * s * up).astype(BF16)
        dg_ref[:, cols], du_ref[:, cols] = by_hidden(gate, up, dact, s)


def hidden(h, dy, full, half):
    tokens, d = h.shape
    ff = full[0].shape[1] // 2
    wide = jax.ShapeDtypeStruct((tokens, ff), BF16)
    return pl.pallas_call(
        hidden_kernel,
        grid=(tokens // ROWS,),
        out_shape=[wide] * 3 + [jax.ShapeDtypeStruct((d, tokens), BF16)] * half,
        in_specs=[rows_of(d), rows_of(d), part_of(full[0], 1, half), part_of(full[1], 1, half), part_of(full[2], 0, half)],
        out_specs=[rows_of(ff)] * 3 + [columns_of(d)] * half,
        compiler_params=params(),
        cost_estimate=pl.CostEstimate(flops=6 * tokens * d * ff, bytes_accessed=4 * tokens * d + 6 * tokens * ff + 6 * d * ff, transcendentals=tokens * ff),
        name="hidden",
    )(h, dy, *full)


def kept_kernel(gate_ref, up_ref, dy_ref, wd_ref, dg_ref, du_ref):
    dy = dy_ref[...]
    for c in range(gate_ref.shape[1] // COLS):
        cols = pl.ds(c * COLS, COLS)
        gate = gate_ref[:, cols]
        dact = dot(dy, wd_ref[cols, :], NT).astype(BF16).astype(F32)
        dg_ref[:, cols], du_ref[:, cols] = by_hidden(gate, up_ref[:, cols], dact, jax.nn.sigmoid(gate))


def kept_hidden(gate, up, dy, full, half):
    tokens, d = dy.shape
    ff = gate.shape[1] // 2
    wide = jax.ShapeDtypeStruct((tokens, ff), BF16)
    block = pl.BlockSpec((ROWS, ff), lambda i: (i, half))
    return pl.pallas_call(
        kept_kernel,
        grid=(tokens // ROWS,),
        out_shape=[wide] * 2,
        in_specs=[block, block, rows_of(d), part_of(full, 0, half)],
        out_specs=[rows_of(ff)] * 2,
        compiler_params=params(),
        cost_estimate=pl.CostEstimate(flops=2 * tokens * d * ff, bytes_accessed=2 * tokens * d + 12 * tokens * ff + 2 * d * ff, transcendentals=tokens * ff),
        name="kept_hidden",
    )(gate, up, dy, full)


def gradient_kernel(turn, counts, at_ref, *refs):
    k = len(counts)
    i, first = pl.program_id(0), 0
    for one, count in enumerate(counts):

        @pl.when(jnp.logical_and(i >= first, i < first + count))
        def _(d_ref=refs[one]):
            out = dot(at_ref[...], d_ref[...])
            refs[k][...] = (out.T if turn else out).astype(BF16)

        first += count


def gradient(at, ds, turn=False):
    rows, tokens = at.shape
    cols = 256
    counts = [d.shape[1] // cols for d in ds]
    firsts = [sum(counts[:one]) for one in range(len(ds))]
    ff = sum(d.shape[1] for d in ds)

    def along(height, one):
        return pl.BlockSpec((height, cols), lambda i: (0, jnp.clip(i - firsts[one], 0, counts[one] - 1)))

    shape, out = (ff, rows), pl.BlockSpec((cols, rows), lambda i: (i, 0))
    if not turn:
        shape, out = (rows, ff), pl.BlockSpec((rows, cols), lambda i: (0, i))
    return pl.pallas_call(
        functools.partial(gradient_kernel, turn, counts),
        grid=(sum(counts),),
        out_shape=jax.ShapeDtypeStruct(shape, BF16),
        in_specs=[whole(at)] + [along(tokens, one) for one in range(len(ds))],
        out_specs=out,
        compiler_params=params(),
        cost_estimate=pl.CostEstimate(flops=2 * tokens * rows * ff, bytes_accessed=2 * (rows * tokens + ff * tokens + rows * ff), transcendentals=0),
        name="gradient",
    )(at, *ds)


LAG = 2


def last_kernel(n, counts, at_ref, *refs):
    k, pieces = len(counts), sum(counts)
    ds, out_ref, own, moving, send_sem, recv_sem = refs[:k], *refs[k:]
    i, me = pl.program_id(0), lax.axis_index("dp")
    right, left = {"dp": lax.rem(me + 1, n)}, {"dp": lax.rem(me + n - 1, n)}
    rows, cols = own.shape[1] // n, own.shape[2] // 2

    def term(piece, side, hop):
        block = lax.rem(me + (1 + hop if side else n - 1 - hop), n)
        return own.at[piece, pl.ds(pl.multiple_of(block * rows, 16), rows), pl.ds(side * cols, cols)]

    def hop_copy(piece, side, hop):
        src = moving.at[hop - 1, side, piece] if hop else term(piece, side, 0)
        return pltpu.make_async_remote_copy(src_ref=src, dst_ref=moving.at[hop, side, piece], send_sem=send_sem.at[hop, side, piece], recv_sem=recv_sem.at[hop, side, piece], device_id=left if side else right, device_id_type=MESH)

    @pl.when(i == 0)
    def _():
        sem = pltpu.get_barrier_semaphore()
        for device in (left, right):
            pl.semaphore_signal(sem, inc=1, device_id=device, device_id_type=MESH)
        pl.semaphore_wait(sem, 2)

    def at_lag(lag):
        return jnp.logical_and(i >= lag, i < lag + pieces)

    for hop in range(1, n):

        @pl.when(at_lag(hop * LAG))
        def _(hop=hop):
            piece = i - hop * LAG
            for side in (0, 1):
                hop_copy(piece, side, hop - 1).wait_recv()
                total = moving[hop - 1, side, piece].astype(F32) + term(piece, side, hop)[...].astype(F32)
                if hop < n - 1:
                    moving[hop - 1, side, piece] = total.astype(BF16)
                else:
                    out_ref[:, side * cols : (side + 1) * cols] = total.astype(BF16)

    first = 0
    for one, count in enumerate(counts):

        @pl.when(jnp.logical_and(i >= first, i < first + count))
        def _(d_ref=ds[one]):
            own[i] = dot(at_ref[...], d_ref[...]).astype(BF16)

        first += count

    for hop in range(n - 1):

        @pl.when(at_lag(hop * LAG))
        def _(hop=hop):
            for side in (0, 1):
                hop_copy(i - hop * LAG, side, hop).start()

    @pl.when(at_lag((n - 1) * LAG))
    def _():
        for hop in range(n - 1):
            for side in (0, 1):
                hop_copy(i - (n - 1) * LAG, side, hop).wait_send()


def last_gradient(n, at, ds):
    (rows, tokens), cols = at.shape, 256
    counts = [d.shape[1] // cols for d in ds]
    firsts = [sum(counts[:one]) for one in range(len(ds))]
    pieces = sum(counts)

    def along(one):
        return pl.BlockSpec((tokens, cols), lambda i: (0, jnp.clip(i - firsts[one], 0, counts[one] - 1)))

    ff = pieces * cols
    return pl.pallas_call(
        functools.partial(last_kernel, n, counts),
        grid=(pieces + (n - 1) * LAG,),
        out_shape=jax.ShapeDtypeStruct((rows // n, ff), BF16),
        in_specs=[whole(at)] + [along(one) for one in range(len(ds))],
        out_specs=pl.BlockSpec((rows // n, cols), lambda i: (0, jnp.clip(i - (n - 1) * LAG, 0, pieces - 1))),
        scratch_shapes=[
            pltpu.VMEM((pieces, rows, cols), BF16),
            pltpu.VMEM((n - 1, 2, pieces, rows // n, cols // 2), BF16),
            pltpu.SemaphoreType.DMA((n - 1, 2, pieces)),
            pltpu.SemaphoreType.DMA((n - 1, 2, pieces)),
        ],
        compiler_params=params(collective_id=3, has_side_effects=True),
        cost_estimate=pl.CostEstimate(flops=4 * tokens * rows * ff, bytes_accessed=2 * (rows * tokens + ff * tokens + rows * ff), transcendentals=0),
        name="last_gradient",
    )(at, *ds)


def states_kernel(dga_ref, dgb_ref, dua_ref, dub_ref, h_ref, dy_ref, wg_ref, wu_ref, dh_ref, dht_ref):
    ff = dga_ref.shape[1]

    def through(a_ref, b_ref, w_ref):
        return (dot(w_ref[:, :ff], a_ref[...], NT) + dot(w_ref[:, ff:], b_ref[...], NT)).astype(BF16)

    da = (through(dga_ref, dgb_ref, wg_ref) + through(dua_ref, dub_ref, wu_ref)).T.astype(F32)
    wide = h_ref[...].astype(F32)
    scale = inv_rms(wide)
    by_scale = jnp.sum(da * wide, -1, keepdims=True)
    dh = da * scale - (by_scale * scale * scale * scale / wide.shape[-1]) * wide
    dh = dy_ref[...] + dh.astype(BF16)
    dh_ref[...] = dh
    dht_ref[...] = dh.T


def states(dg, du, h, dy, full):
    tokens, d = h.shape
    ff = dg[0].shape[1]
    return pl.pallas_call(
        states_kernel,
        grid=(tokens // ROWS,),
        out_shape=[jax.ShapeDtypeStruct((tokens, d), BF16), jax.ShapeDtypeStruct((d, tokens), BF16)],
        in_specs=[rows_of(ff)] * 4 + [rows_of(d), rows_of(d), whole(full[0]), whole(full[1])],
        out_specs=[rows_of(d), columns_of(d)],
        compiler_params=params(),
        cost_estimate=pl.CostEstimate(flops=8 * tokens * d * ff, bytes_accessed=8 * tokens * ff + 8 * tokens * d + 8 * d * ff, transcendentals=tokens),
        name="states",
    )(*dg, *du, h, dy, full[0], full[1])


def clip_kernel(n, count, *refs):
    sums, (out_ref, parts, send_sem, recv_sem) = refs[:-4], refs[-4:]
    me = lax.axis_index("dp")
    others = [{"dp": lax.rem(me + away, n)} for away in range(1, n)]
    barrier = pltpu.get_barrier_semaphore()
    for device in others:
        pl.semaphore_signal(barrier, inc=1, device_id=device, device_id_type=MESH)
    mine = jnp.zeros((8, 128), F32)
    for ref in sums:
        rows, columns = ref.shape

        def more(r, total, ref=ref):
            wide = ref[pl.ds(pl.multiple_of(r * 16, 16), 16)].astype(F32)
            return total + wide * wide

        mine = mine + jnp.sum(lax.fori_loop(0, rows // 16, more, jnp.zeros((16, columns), F32)))
    parts[me] = mine
    pl.semaphore_wait(barrier, n - 1)
    copies = [
        pltpu.make_async_remote_copy(src_ref=parts.at[me], dst_ref=parts.at[me], send_sem=send_sem.at[k], recv_sem=recv_sem.at[k], device_id=device, device_id_type=MESH)
        for k, device in enumerate(others)
    ]
    for copy in copies:
        copy.start()
    for copy in copies:
        copy.wait()
    total = parts[0]
    for k in range(1, n):
        total = total + parts[k]
    out_ref[...] = jnp.minimum(1.0, 0.5 * lax.rsqrt(total / count + 1e-30))


def clip_factor(n, sums):
    count = n * sum(g.size for g in sums)
    vmem = pl.BlockSpec(memory_space=pltpu.VMEM)
    return pl.pallas_call(
        functools.partial(clip_kernel, n, count),
        out_shape=jax.ShapeDtypeStruct((8, 128), F32),
        in_specs=[vmem] * len(sums),
        out_specs=vmem,
        scratch_shapes=[pltpu.VMEM((n, 8, 128), F32), pltpu.SemaphoreType.DMA((n - 1,)), pltpu.SemaphoreType.DMA((n - 1,))],
        compiler_params=pltpu.CompilerParams(collective_id=4, has_side_effects=True, vmem_limit_bytes=32 * 1024 * 1024),
        cost_estimate=pl.CostEstimate(flops=2 * count, bytes_accessed=2 * count // n, transcendentals=0),
        name="clip_factor",
    )(*sums)[0, 0]


def adamw(w, m, v, g):
    m = 0.9 * m + 0.1 * g
    v = 0.95 * v + 0.05 * g * g
    step = m * lax.rsqrt(v + 1e-8) + 0.1 * w
    return (w - 0.02 * step).astype(BF16), m, v


def solution(mesh):
    n = mesh.shape["dp"]

    def scattered(g):
        return lax.psum_scatter(g, "dp", scatter_dimension=0, tiled=True)

    def follow(array, *earlier):
        return lax.optimization_barrier((array, *earlier))[0]

    def step(x, dy, *arrays):
        weights, m, v = (arrays[i : i + 3] for i in (0, 3, 6))
        x, dy = x[0], dy[0]
        w_gate, w_up, w_down = weights
        full = gathered(n, (w_gate, w_up))
        gate, up, act, at0, down0, gate1, up1 = up_part(n, x, full, (w_down, w_gate, w_up), (0, 1, 1))
        h, at1, down1 = down_part(n, x, act, down0, (w_down,), (1,))
        full1 = gate1, up1, down1

        act_a, dg_a, du_a = hidden(h, dy, full1, 0)
        one_a = gradient(at1, (dg_a, du_a))
        sum_a = scattered(one_a)
        act_b, dg_b, du_b, dyt = hidden(follow(h, one_a), dy, full1, 1)
        one_b = gradient(at1, (dg_b, du_b))
        sum_b = scattered(one_b)
        one_down = gradient(follow(dyt, one_b), (act_a, act_b), True)
        sum_down = scattered(one_down)
        dh, dht = states((dg_a, dg_b), (du_a, du_b), follow(h, one_down, sum_a), dy, full1)
        down = gradient(dht, (act,), True)
        last_down = scattered(down)
        dg_a, du_a = kept_hidden(gate, up, follow(dh, down, sum_b), down0, 0)
        a = gradient(at0, (dg_a, du_a))
        last_a = scattered(a)
        dg_b, du_b = kept_hidden(gate, up, follow(dh, a, sum_down), down0, 1)
        last_b = last_gradient(n, follow(at0, last_down), (dg_b, du_b))
        last_a = follow(last_a, last_b)

        sums = sum_a, sum_b, sum_down, last_down, last_a, last_b
        factor = clip_factor(n, sums)

        def joined(a, b, side):
            half = a.shape[1] // 2
            return jnp.concatenate([one[:, side * half : (side + 1) * half] for one in (a, b)], -1)

        pairs = (last_a, last_b), (sum_a, sum_b)
        gradients = [jnp.stack([joined(a, b, side) for a, b in pairs]).astype(F32) for side in range(2)]
        gradients.append(jnp.stack([last_down, sum_down]).astype(F32))
        gradients = [g * factor for g in gradients]
        new = [adamw(w.astype(F32), m, v, g) for w, m, v, g in zip(weights, m, v, gradients, strict=True)]
        return tuple(one[which] for which in range(3) for one in new)

    spec, cut = P(("rep", "dp"), None, None), P(None, "dp", None)
    return jax.shard_map(
        step,
        mesh=mesh,
        in_specs=(spec, spec) + (cut,) * 9,
        out_specs=(P("rep", "dp", None),) * 9,
        check_vma=False,
    )
```

```python
import functools

import jax
import jax.numpy as jnp
from jax import lax
from jax.experimental import pallas as pl
from jax.experimental.pallas import tpu as pltpu
from jax.sharding import PartitionSpec as P

MESH = pl.DeviceIdType.MESH
ANY = pl.BlockSpec(memory_space=pl.ANY)
F32, BF16 = jnp.float32, jnp.bfloat16
VMEM_LIMIT = 60 * 1024 * 1024
ROWS = 512
COLS = 256
EARLY = 1024


def dot(a, b, dims=((1,), (0,))):
    return lax.dot_general(a, b, (dims, ((), ())), preferred_element_type=F32)


NT = ((1,), (1,))


def inv_rms(wide):
    return lax.rsqrt(jnp.mean(wide * wide, -1, keepdims=True) + 1e-6)


def normed(h):
    wide = h.astype(F32)
    return (wide * inv_rms(wide)).astype(BF16)


class Gather:
    def __init__(self, n, shards, fulls, stages, local_sem, send_sem, recv_sem):
        self.me, rep = lax.axis_index("dp"), lax.axis_index("rep")
        self.n, self.p, self.b = n, lax.rem(rep, 2), lax.rem(rep // 2, 2)
        self.right, self.left = {"dp": lax.rem(self.me + 1, n)}, {"dp": lax.rem(self.me + n - 1, n)}
        self.partner, self.sharer = {"rep": rep + 1 - 2 * self.p}, {"rep": rep + 2 - 4 * self.b}
        self.shards, self.fulls, self.stages = shards, fulls, stages
        self.local_sem, self.send_sem, self.recv_sem = local_sem, send_sem, recv_sem

    def barrier(self):
        sem = pltpu.get_barrier_semaphore()
        for device in (self.left, self.right, self.partner, self.sharer):
            pl.semaphore_signal(sem, inc=1, device_id=device, device_id_type=MESH)
        pl.semaphore_wait(sem, 4)

    def cut(self, k):
        rows, columns = self.shards[k].shape
        wide = columns % 256 == 0
        unit = 128 if wide else 16
        units = columns // unit if wide else rows // 2 // unit
        alone = units * 3 // 10
        return wide, unit, alone, units - 2 * alone

    def place(self, ref, row, k, start, size):
        wide, unit, _, _ = self.cut(k)
        if wide:
            return ref.at[pl.ds(pl.multiple_of(row, 16), self.shards[k].shape[0] // 2), pl.ds(pl.multiple_of(start * unit, unit), size * unit)]
        return ref.at[pl.ds(pl.multiple_of(row + start * unit, 16), size * unit)]

    def there(self, k, away, start, size):
        rows = self.shards[k].shape[0]
        owner = lax.rem(self.me + away + self.n, self.n)
        return self.place(self.fulls[k], owner * rows + self.p * (rows // 2), k, start, size)

    def copy(self, k, slot, src, dst, device):
        return pltpu.make_async_remote_copy(src_ref=src, dst_ref=dst, send_sem=self.send_sem.at[k, slot], recv_sem=self.recv_sem.at[k, slot], device_id=device, device_id_type=MESH)

    def first(self, k, side):
        _, _, alone, both = self.cut(k)
        own = self.place(self.shards[k], self.p * (self.shards[k].shape[0] // 2), k, self.b * alone, alone + both)
        return self.copy(k, side, own, self.there(k, 0, self.b * alone, alone + both), self.left if side else self.right)

    def second(self, k, side):
        _, _, alone, both = self.cut(k)
        size = (alone + both + 1) // 2
        start = self.b * alone + (size if side else 0)
        place = self.there(k, 1 if side else -1, start, alone + both - size if side else size)
        return self.copy(k, 2 + side, place, place, self.left if side else self.right)

    def shared(self, k, which):
        _, _, alone, both = self.cut(k)
        place = self.there(k, (-1, 1, 2)[which], self.b * (alone + both), alone)
        return self.copy(k, 4 + which, place, place, self.sharer)

    def over(self, k, which):
        _, _, alone, both = self.cut(k)
        away = (-1, 1, 2)[which % 3]
        if which < 3:
            place = self.there(k, away, self.b * alone, alone + both)
        else:
            place = self.there(k, away, (1 - self.b) * (alone + both), alone)
        return self.copy(k, 7 + which, place, place, self.partner)

    def load(self, k):
        return pltpu.make_async_copy(self.shards[k], self.stages[k], self.local_sem.at[k, 0])

    def store(self, k):
        rows = self.shards[k].shape[0]
        place = self.fulls[k].at[pl.ds(pl.multiple_of(self.me * rows, 16), rows)]
        return pltpu.make_async_copy(self.stages[k], place, self.local_sem.at[k, 1])

    def start(self, k):
        self.first(k, 0).start()
        self.first(k, 1).start()
        self.load(k).start()

    def keep(self, k):
        self.load(k).wait()
        self.store(k).start()

    def forward(self, k):
        for side in (0, 1):
            self.first(k, side).wait_recv()
            self.second(k, side).start()
            self.shared(k, side).start()
            self.over(k, side).start()

    def last(self, k):
        self.second(k, 0).wait_recv()
        self.second(k, 1).wait_recv()
        self.shared(k, 2).start()
        self.over(k, 2).start()
        for side in (0, 1):
            self.shared(k, side).wait_recv()
            self.over(k, 3 + side).start()

    def end(self, k):
        self.shared(k, 2).wait_recv()
        self.over(k, 5).start()

    def finish(self, k):
        self.store(k).wait()
        for which in range(6):
            self.over(k, which).wait()
        for side in (0, 1):
            self.first(k, side).wait_send()
            self.second(k, side).wait_send()
        for which in range(3):
            self.shared(k, which).wait_send()


def gather_scratch(weights, pieces=1):
    k = len(weights) * pieces
    return [pltpu.VMEM(w.shape[1:], w.dtype) for w in weights] + [pltpu.SemaphoreType.DMA((k, 2)), pltpu.SemaphoreType.DMA((k, 13)), pltpu.SemaphoreType.DMA((k, 13))]


def fulls_of(n, weights):
    return [jax.ShapeDtypeStruct((n * w.shape[1], w.shape[2]), w.dtype) for w in weights]


def gather_kernel(n, *refs):
    k = (len(refs) - 3) // 3
    columns = refs[0].shape[2] // 2
    halves = [pl.ds(half * columns, columns) for half in range(2)]
    shards = [s.at[0, :, half] for s in refs[:k] for half in halves]
    fulls, stages = ([s.at[:, half] for s in some for half in halves] for some in (refs[k : 2 * k], refs[2 * k : 3 * k]))
    g = Gather(n, shards, fulls, stages, *refs[3 * k :])
    g.barrier()
    for phase in (g.start, g.keep, g.forward, g.last, g.end, g.finish):
        for one in range(2 * k):
            phase(one)


def gathered(n, weights):
    k = len(weights)
    sent = sum(3 * w.shape[1] * w.shape[2] for w in weights)
    return pl.pallas_call(
        functools.partial(gather_kernel, n),
        out_shape=fulls_of(n, weights),
        in_specs=[ANY] * k,
        out_specs=[ANY] * k,
        scratch_shapes=gather_scratch(weights, 2),
        compiler_params=pltpu.CompilerParams(collective_id=0, has_side_effects=True, vmem_limit_bytes=VMEM_LIMIT),
        cost_estimate=pl.CostEstimate(flops=40_000_000_000, bytes_accessed=8 * sent, transcendentals=0),
        name="gather",
    )(*weights)


def whole(array):
    return pl.BlockSpec(array.shape, lambda i: (0,) * len(array.shape), pipeline_mode=pl.Buffered(1))


def rows_of(d):
    return pl.BlockSpec((ROWS, d), lambda i: (i, 0))


def columns_of(d):
    return pl.BlockSpec((d, ROWS), lambda i: (0, i))


def part_of(array, dim, half):
    shape = tuple(s // 2 if i == dim else s for i, s in enumerate(array.shape))
    place = tuple(half if i == dim else 0 for i in range(2))
    return pl.BlockSpec(shape, lambda i: place, pipeline_mode=pl.Buffered(1))


def params(**more):
    return pltpu.CompilerParams(dimension_semantics=("arbitrary",), vmem_limit_bytes=VMEM_LIMIT, **more)


def beside(g, k, steps, times):
    i = pl.program_id(0)
    phases = (g.start, (0,) * k), (g.keep, (1,) * k), *zip((g.forward, g.last), times)
    for phase, steps_of in phases:
        for one, at in enumerate(steps_of):

            @pl.when(i == at)
            def _(phase=phase, one=one):
                if phase == g.start and one == 0:
                    g.barrier()
                phase(one)


def after(g, k, steps):
    @pl.when(pl.program_id(0) == steps - 1)
    def _():
        for phase in (g.end, g.finish):
            for one in range(k):
                phase(one)


def up_kernel(n, layers, steps, x_ref, wg_ref, wu_ref, *refs):
    k = len(layers)
    shards, (*kept, act_ref, at_ref), refs = refs[:k], refs[k : k + 6], refs[k + 6 :]
    g = Gather(n, [s.at[layer] for s, layer in zip(shards, layers)], refs[:k], refs[k : 2 * k], *refs[2 * k :])
    beside(g, k, steps, ((2, 3, 4), (5, 6, 7)))
    a = normed(x_ref[...])
    at_ref[...] = a.T
    for c in range(wg_ref.shape[1] // COLS):
        cols = pl.ds(c * COLS, COLS)
        gate = dot(a, wg_ref[:, cols])
        up = dot(a, wu_ref[:, cols])
        late = c * COLS >= EARLY
        there = pl.ds(c * COLS - EARLY * late, COLS)
        kept[late][:, there] = gate
        kept[2 + late][:, there] = up
        act_ref[:, cols] = (gate * jax.nn.sigmoid(gate) * up).astype(BF16)
    after(g, k, steps)


def up_part(n, x, full, weights, layers):
    tokens, d = x.shape
    ff, k = full[0].shape[1], len(weights)
    steps = tokens // ROWS
    widths = (EARLY, ff - EARLY) * 2
    return pl.pallas_call(
        functools.partial(up_kernel, n, layers, steps),
        grid=(steps,),
        out_shape=[*(jax.ShapeDtypeStruct((tokens, width), F32) for width in widths), jax.ShapeDtypeStruct((tokens, ff), BF16), jax.ShapeDtypeStruct((d, tokens), BF16), *fulls_of(n, weights)],
        in_specs=[rows_of(d), whole(full[0]), whole(full[1])] + [ANY] * k,
        out_specs=[*(rows_of(width) for width in widths), rows_of(ff), columns_of(d)] + [ANY] * k,
        scratch_shapes=gather_scratch(weights),
        compiler_params=params(collective_id=1, has_side_effects=True),
        cost_estimate=pl.CostEstimate(flops=4 * tokens * d * ff, bytes_accessed=10 * tokens * ff, transcendentals=tokens * ff),
        name="up",
    )(x, *full, *weights)


def down_kernel(n, layers, steps, x_ref, act_ref, wd_ref, *refs):
    k = len(layers)
    shards, (h_ref, at_ref), refs = refs[:k], refs[k : k + 2], refs[k + 2 :]
    g = Gather(n, [s.at[layer] for s, layer in zip(shards, layers)], refs[:k], refs[k : 2 * k], *refs[2 * k :])
    beside(g, k, steps, ((3,), (6,)))
    h = x_ref[...] + dot(act_ref[...], wd_ref[...]).astype(BF16)
    h_ref[...] = h
    at_ref[...] = normed(h).T
    after(g, k, steps)


def down_part(n, x, act, full, weights, layers):
    tokens, d = x.shape
    ff, k = act.shape[1], len(weights)
    steps = tokens // ROWS
    return pl.pallas_call(
        functools.partial(down_kernel, n, layers, steps),
        grid=(steps,),
        out_shape=[jax.ShapeDtypeStruct((tokens, d), BF16), jax.ShapeDtypeStruct((d, tokens), BF16), *fulls_of(n, weights)],
        in_specs=[rows_of(d), rows_of(ff), whole(full)] + [ANY] * k,
        out_specs=[rows_of(d), columns_of(d)] + [ANY] * k,
        scratch_shapes=gather_scratch(weights),
        compiler_params=params(collective_id=2, has_side_effects=True),
        cost_estimate=pl.CostEstimate(flops=2 * tokens * d * ff, bytes_accessed=2 * tokens * ff + 6 * tokens * d, transcendentals=0),
        name="down",
    )(x, act, full, *weights)


def by_hidden(gate, up, dact, s):
    silu = gate * s
    return (dact * up * (s + silu * (1 - s))).astype(BF16), (dact * silu).astype(BF16)


def hidden_kernel(h_ref, dy_ref, wg_ref, wu_ref, wd_ref, act_ref, dg_ref, du_ref, *dyt_ref):
    a, dy = normed(h_ref[...]), dy_ref[...]
    for ref in dyt_ref:
        ref[...] = dy.T
    for c in range(wg_ref.shape[1] // COLS):
        cols = pl.ds(c * COLS, COLS)
        gate = dot(a, wg_ref[:, cols])
        up = dot(a, wu_ref[:, cols])
        dact = dot(dy, wd_ref[cols, :], NT).astype(BF16).astype(F32)
        s = jax.nn.sigmoid(gate)
        act_ref[:, cols] = (gate * s * up).astype(BF16)
        dg_ref[:, cols], du_ref[:, cols] = by_hidden(gate, up, dact, s)


def hidden(h, dy, full, half):
    tokens, d = h.shape
    ff = full[0].shape[1] // 2
    wide = jax.ShapeDtypeStruct((tokens, ff), BF16)
    return pl.pallas_call(
        hidden_kernel,
        grid=(tokens // ROWS,),
        out_shape=[wide] * 3 + [jax.ShapeDtypeStruct((d, tokens), BF16)] * half,
        in_specs=[rows_of(d), rows_of(d), part_of(full[0], 1, half), part_of(full[1], 1, half), part_of(full[2], 0, half)],
        out_specs=[rows_of(ff)] * 3 + [columns_of(d)] * half,
        compiler_params=params(),
        cost_estimate=pl.CostEstimate(flops=6 * tokens * d * ff, bytes_accessed=4 * tokens * d + 6 * tokens * ff + 6 * d * ff, transcendentals=tokens * ff),
        name="hidden",
    )(h, dy, *full)


def kept_kernel(start, gate_ref, up_ref, dy_ref, wd_ref, dg_ref, du_ref):
    dy = dy_ref[...]
    for c in range(gate_ref.shape[1] // COLS):
        cols = pl.ds(c * COLS, COLS)
        gate = gate_ref[:, cols]
        dact = dot(dy, wd_ref[pl.ds(start + c * COLS, COLS), :], NT).astype(BF16).astype(F32)
        dg_ref[:, cols], du_ref[:, cols] = by_hidden(gate, up_ref[:, cols], dact, jax.nn.sigmoid(gate))


def kept_hidden(gate, up, dy, full, start):
    tokens, d = dy.shape
    ff = gate.shape[1]
    wide = jax.ShapeDtypeStruct((tokens, ff), BF16)
    return pl.pallas_call(
        functools.partial(kept_kernel, start),
        grid=(tokens // ROWS,),
        out_shape=[wide] * 2,
        in_specs=[rows_of(ff), rows_of(ff), rows_of(d), whole(full)],
        out_specs=[rows_of(ff)] * 2,
        compiler_params=params(),
        cost_estimate=pl.CostEstimate(flops=2 * tokens * d * ff, bytes_accessed=2 * tokens * d + 12 * tokens * ff + 2 * d * ff, transcendentals=tokens * ff),
        name="kept_hidden",
    )(gate, up, dy, full)


def gradient_kernel(turn, counts, at_ref, *refs):
    k = len(counts)
    i, first = pl.program_id(0), 0
    for one, count in enumerate(counts):

        @pl.when(jnp.logical_and(i >= first, i < first + count))
        def _(d_ref=refs[one]):
            out = dot(at_ref[...], d_ref[...])
            refs[k][...] = (out.T if turn else out).astype(BF16)

        first += count


def gradient(at, ds, turn=False):
    rows, tokens = at.shape
    cols = 256
    counts = [d.shape[1] // cols for d in ds]
    firsts = [sum(counts[:one]) for one in range(len(ds))]
    ff = sum(d.shape[1] for d in ds)

    def along(height, one):
        return pl.BlockSpec((height, cols), lambda i: (0, jnp.clip(i - firsts[one], 0, counts[one] - 1)))

    shape, out = (ff, rows), pl.BlockSpec((cols, rows), lambda i: (i, 0))
    if not turn:
        shape, out = (rows, ff), pl.BlockSpec((rows, cols), lambda i: (0, i))
    return pl.pallas_call(
        functools.partial(gradient_kernel, turn, counts),
        grid=(sum(counts),),
        out_shape=jax.ShapeDtypeStruct(shape, BF16),
        in_specs=[whole(at)] + [along(tokens, one) for one in range(len(ds))],
        out_specs=out,
        compiler_params=params(),
        cost_estimate=pl.CostEstimate(flops=2 * tokens * rows * ff, bytes_accessed=2 * (rows * tokens + ff * tokens + rows * ff), transcendentals=0),
        name="gradient",
    )(at, *ds)


LAG = 2


def last_kernel(n, counts, at_ref, *refs):
    k, pieces = len(counts), sum(counts)
    ds, out_ref, own, moving, send_sem, recv_sem = refs[:k], *refs[k:]
    i, me = pl.program_id(0), lax.axis_index("dp")
    right, left = {"dp": lax.rem(me + 1, n)}, {"dp": lax.rem(me + n - 1, n)}
    rows, cols = own.shape[1] // n, own.shape[2] // 2

    def term(piece, side, hop):
        block = lax.rem(me + (1 + hop if side else n - 1 - hop), n)
        return own.at[piece, pl.ds(pl.multiple_of(block * rows, 16), rows), pl.ds(side * cols, cols)]

    def hop_copy(piece, side, hop):
        src = moving.at[hop - 1, side, piece] if hop else term(piece, side, 0)
        return pltpu.make_async_remote_copy(src_ref=src, dst_ref=moving.at[hop, side, piece], send_sem=send_sem.at[hop, side, piece], recv_sem=recv_sem.at[hop, side, piece], device_id=left if side else right, device_id_type=MESH)

    @pl.when(i == 0)
    def _():
        sem = pltpu.get_barrier_semaphore()
        for device in (left, right):
            pl.semaphore_signal(sem, inc=1, device_id=device, device_id_type=MESH)
        pl.semaphore_wait(sem, 2)

    def at_lag(lag):
        return jnp.logical_and(i >= lag, i < lag + pieces)

    for hop in range(1, n):

        @pl.when(at_lag(hop * LAG))
        def _(hop=hop):
            piece = i - hop * LAG
            for side in (0, 1):
                hop_copy(piece, side, hop - 1).wait_recv()
                total = moving[hop - 1, side, piece].astype(F32) + term(piece, side, hop)[...].astype(F32)
                if hop < n - 1:
                    moving[hop - 1, side, piece] = total.astype(BF16)
                else:
                    out_ref[:, side * cols : (side + 1) * cols] = total.astype(BF16)

    first = 0
    for one, count in enumerate(counts):

        @pl.when(jnp.logical_and(i >= first, i < first + count))
        def _(d_ref=ds[one]):
            own[i] = dot(at_ref[...], d_ref[...]).astype(BF16)

        first += count

    for hop in range(n - 1):

        @pl.when(at_lag(hop * LAG))
        def _(hop=hop):
            for side in (0, 1):
                hop_copy(i - hop * LAG, side, hop).start()

    @pl.when(at_lag((n - 1) * LAG))
    def _():
        for hop in range(n - 1):
            for side in (0, 1):
                hop_copy(i - (n - 1) * LAG, side, hop).wait_send()


def last_gradient(n, at, ds):
    (rows, tokens), cols = at.shape, 256
    counts = [d.shape[1] // cols for d in ds]
    firsts = [sum(counts[:one]) for one in range(len(ds))]
    pieces = sum(counts)

    def along(one):
        return pl.BlockSpec((tokens, cols), lambda i: (0, jnp.clip(i - firsts[one], 0, counts[one] - 1)))

    ff = pieces * cols
    return pl.pallas_call(
        functools.partial(last_kernel, n, counts),
        grid=(pieces + (n - 1) * LAG,),
        out_shape=jax.ShapeDtypeStruct((rows // n, ff), BF16),
        in_specs=[whole(at)] + [along(one) for one in range(len(ds))],
        out_specs=pl.BlockSpec((rows // n, cols), lambda i: (0, jnp.clip(i - (n - 1) * LAG, 0, pieces - 1))),
        scratch_shapes=[
            pltpu.VMEM((pieces, rows, cols), BF16),
            pltpu.VMEM((n - 1, 2, pieces, rows // n, cols // 2), BF16),
            pltpu.SemaphoreType.DMA((n - 1, 2, pieces)),
            pltpu.SemaphoreType.DMA((n - 1, 2, pieces)),
        ],
        compiler_params=params(collective_id=3, has_side_effects=True),
        cost_estimate=pl.CostEstimate(flops=4 * tokens * rows * ff, bytes_accessed=2 * (rows * tokens + ff * tokens + rows * ff), transcendentals=0),
        name="last_gradient",
    )(at, *ds)


def states_kernel(dga_ref, dgb_ref, dua_ref, dub_ref, h_ref, dy_ref, wg_ref, wu_ref, dh_ref, dht_ref):
    ff = dga_ref.shape[1]

    def through(a_ref, b_ref, w_ref):
        return (dot(w_ref[:, :ff], a_ref[...], NT) + dot(w_ref[:, ff:], b_ref[...], NT)).astype(BF16)

    da = (through(dga_ref, dgb_ref, wg_ref) + through(dua_ref, dub_ref, wu_ref)).T.astype(F32)
    wide = h_ref[...].astype(F32)
    scale = inv_rms(wide)
    by_scale = jnp.sum(da * wide, -1, keepdims=True)
    dh = da * scale - (by_scale * scale * scale * scale / wide.shape[-1]) * wide
    dh = dy_ref[...] + dh.astype(BF16)
    dh_ref[...] = dh
    dht_ref[...] = dh.T


def states(dg, du, h, dy, full):
    tokens, d = h.shape
    ff = dg[0].shape[1]
    return pl.pallas_call(
        states_kernel,
        grid=(tokens // ROWS,),
        out_shape=[jax.ShapeDtypeStruct((tokens, d), BF16), jax.ShapeDtypeStruct((d, tokens), BF16)],
        in_specs=[rows_of(ff)] * 4 + [rows_of(d), rows_of(d), whole(full[0]), whole(full[1])],
        out_specs=[rows_of(d), columns_of(d)],
        compiler_params=params(),
        cost_estimate=pl.CostEstimate(flops=8 * tokens * d * ff, bytes_accessed=8 * tokens * ff + 8 * tokens * d + 8 * d * ff, transcendentals=tokens),
        name="states",
    )(*dg, *du, h, dy, full[0], full[1])


def clip_kernel(n, count, *refs):
    sums, (out_ref, parts, send_sem, recv_sem) = refs[:-4], refs[-4:]
    me = lax.axis_index("dp")
    others = [{"dp": lax.rem(me + away, n)} for away in range(1, n)]
    barrier = pltpu.get_barrier_semaphore()
    for device in others:
        pl.semaphore_signal(barrier, inc=1, device_id=device, device_id_type=MESH)
    mine = jnp.zeros((8, 128), F32)
    for ref in sums:
        rows, columns = ref.shape

        def more(r, total, ref=ref):
            wide = ref[pl.ds(pl.multiple_of(r * 16, 16), 16)].astype(F32)
            return total + wide * wide

        mine = mine + jnp.sum(lax.fori_loop(0, rows // 16, more, jnp.zeros((16, columns), F32)))
    parts[me] = mine
    pl.semaphore_wait(barrier, n - 1)
    copies = [
        pltpu.make_async_remote_copy(src_ref=parts.at[me], dst_ref=parts.at[me], send_sem=send_sem.at[k], recv_sem=recv_sem.at[k], device_id=device, device_id_type=MESH)
        for k, device in enumerate(others)
    ]
    for copy in copies:
        copy.start()
    for copy in copies:
        copy.wait()
    total = parts[0]
    for k in range(1, n):
        total = total + parts[k]
    out_ref[...] = jnp.minimum(1.0, 0.5 * lax.rsqrt(total / count + 1e-30))


def clip_factor(n, sums):
    count = n * sum(g.size for g in sums)
    vmem = pl.BlockSpec(memory_space=pltpu.VMEM)
    return pl.pallas_call(
        functools.partial(clip_kernel, n, count),
        out_shape=jax.ShapeDtypeStruct((8, 128), F32),
        in_specs=[vmem] * len(sums),
        out_specs=vmem,
        scratch_shapes=[pltpu.VMEM((n, 8, 128), F32), pltpu.SemaphoreType.DMA((n - 1,)), pltpu.SemaphoreType.DMA((n - 1,))],
        compiler_params=pltpu.CompilerParams(collective_id=4, has_side_effects=True, vmem_limit_bytes=32 * 1024 * 1024),
        cost_estimate=pl.CostEstimate(flops=2 * count, bytes_accessed=2 * count // n, transcendentals=0),
        name="clip_factor",
    )(*sums)[0, 0]


def adamw(w, m, v, g):
    m = 0.9 * m + 0.1 * g
    v = 0.95 * v + 0.05 * g * g
    step = m * lax.rsqrt(v + 1e-8) + 0.1 * w
    return (w - 0.02 * step).astype(BF16), m, v


def solution(mesh):
    n = mesh.shape["dp"]

    def scattered(g):
        return lax.psum_scatter(g, "dp", scatter_dimension=0, tiled=True)

    def follow(array, *earlier):
        return lax.optimization_barrier((array, *earlier))[0]

    def step(x, dy, *arrays):
        weights, m, v = (arrays[i : i + 3] for i in (0, 3, 6))
        x, dy = x[0], dy[0]
        w_gate, w_up, w_down = weights
        full = gathered(n, (w_gate, w_up))
        gate_a, gate_b, up_a, up_b, act, at0, down0, gate1, up1 = up_part(n, x, full, (w_down, w_gate, w_up), (0, 1, 1))
        h, at1, down1 = down_part(n, x, act, down0, (w_down,), (1,))
        full1 = gate1, up1, down1

        act_a, dg_a, du_a = hidden(h, dy, full1, 0)
        one_a = gradient(at1, (dg_a, du_a))
        sum_a = scattered(one_a)
        act_b, dg_b, du_b, dyt = hidden(follow(h, one_a), dy, full1, 1)
        one_b = gradient(at1, (dg_b, du_b))
        sum_b = scattered(one_b)
        one_down = gradient(follow(dyt, one_b), (act_a, act_b), True)
        sum_down = scattered(one_down)
        dh, dht = states((dg_a, dg_b), (du_a, du_b), follow(h, one_down, sum_a), dy, full1)
        down = gradient(dht, (act,), True)
        last_down = scattered(down)
        dg_a, du_a = kept_hidden(gate_a, up_a, follow(dh, down, sum_b), down0, 0)
        a = gradient(at0, (dg_a, du_a))
        last_a = scattered(a)
        dg_b, du_b = kept_hidden(gate_b, up_b, follow(dh, a, sum_down), down0, EARLY)
        last_b = last_gradient(n, follow(at0, last_down), (dg_b, du_b))
        last_a = follow(last_a, last_b)

        sums = sum_a, sum_b, sum_down, last_down, last_a, last_b
        factor = clip_factor(n, sums)

        def joined(a, b, side):
            return jnp.concatenate([jnp.split(one, 2, -1)[side] for one in (a, b)], -1)

        pairs = (last_a, last_b), (sum_a, sum_b)
        gradients = [jnp.stack([joined(a, b, side) for a, b in pairs]).astype(F32) for side in range(2)]
        gradients.append(jnp.stack([last_down, sum_down]).astype(F32))
        gradients = [g * factor for g in gradients]
        new = [adamw(w.astype(F32), m, v, g) for w, m, v, g in zip(weights, m, v, gradients, strict=True)]
        return tuple(one[which] for which in range(3) for one in new)

    spec, cut = P(("rep", "dp"), None, None), P(None, "dp", None)
    return jax.shard_map(
        step,
        mesh=mesh,
        in_specs=(spec, spec) + (cut,) * 9,
        out_specs=(P("rep", "dp", None),) * 9,
        check_vma=False,
    )
```
